32 devices in a mesh: beam: 2 (over x), tm: 16 (over z, y, core).
Axes of the slice: x: 2, y: 2, z: 4, core: 2. Of those that a mesh axis runs over, the one named last changes fastest.
Arguments:
- voltage: bfloat16 [2, 2, 2097152], P(None, None, ('beam', 'tm')), parts along dimension 2, may hold values from -11 to 11
- delays: int32 [64, 2048], replicated, may hold values from 0 to 96, as said below
- chan_mask: int32 [4096], P('beam'), parts along dimension 0, may hold values 0 or 1
Outputs:
- zscore: float32 [64, 1024], P(None, ('beam', 'tm')), parts along dimension 1
- trial_stats: float32 [3, 128], P(None, 'beam'), parts along dimension 1
The draws below stay inside these ranges and needn't reach their ends.
There are 2 independent parts, one for each index of `beam`. The reference program is written for one: setup_inputs(seed, part) draws one part's arguments, and reference() takes and returns one part's arrays. A program takes and returns all parts, laid end to end along the dimension named above; an argument that names none is the same for every part. Nothing has to cross between parts.
Inputs may be any that keep to these rules, and one draw needn't show every extreme that they name: For each trial the delays never rise from one channel to the next; the last channel's delays are 0, and the first channel's delay of some trial is 96.
All inputs are finite; a program needn't handle non-finite values.
Results may differ from the reference program's by a relative error of at most 0.002.
Values may be sent and summed in bfloat16 or wider, within the bound.
No kernel may reach another device: no remote copies, remote signals or barrier semaphores. Data moves between devices by JAX's collectives and lax.ppermute only.
A program may use at most 64 MiB of HBM per device.

```python
import jax
import jax.numpy as jnp
from jax import lax

NCHAN = 2048
TAPS = 16
NDM = 64
SAMPLES = 1048576
MAXD = 96


def draw_voltage(key, part):
    noise_key = jax.random.fold_in(jax.random.fold_in(key, 11), 0)
    position = jnp.arange(SAMPLES, dtype=jnp.float32) / SAMPLES
    envelope = jnp.exp(0.5 * jnp.log(3.5) * position)
    values = jnp.clip(jax.random.normal(noise_key, (2, 2, SAMPLES), jnp.float32) * envelope, -11.0, 11.0)
    return values.astype(jnp.bfloat16)


def draw_delays(key, part):
    size_key, pick_key = jax.random.split(jax.random.fold_in(key, 23))
    reaches = jax.random.randint(size_key, (NDM,), 0, MAXD + 1)
    chosen = jax.random.randint(pick_key, (), 0, NDM)
    reaches = jnp.where(jnp.arange(NDM, dtype=jnp.int32) == chosen, MAXD, reaches)
    channel = jnp.arange(NCHAN, dtype=jnp.int32)
    scale_unit = max(1, (NCHAN - 1) * 3 * NCHAN // 4096)
    chan_curve = (NCHAN - 1 - channel) * (3 * NCHAN - channel) // scale_unit
    top_value = (NCHAN - 1) * 3 * NCHAN // scale_unit
    return (reaches[:, None] * chan_curve[None, :] // top_value).astype(jnp.int32)


def plant(array, rng, least, high):
    shape = array.shape
    place = [jax.random.randint(jax.random.fold_in(rng, axis), (), 0, shape[axis]) for axis in range(len(shape))]
    array = array.at[tuple(place)].set(least)
    longest = shape.index(max(shape))
    place[longest] = (place[longest] + 1) % shape[longest]
    return array.at[tuple(place)].set(high)


def setup_inputs(seed: int = 0, part: int = 0) -> dict:
    key_of = jax.random.split(jax.random.key(seed), 4)
    part_splits = jax.random.split(jax.random.fold_in(key_of[3], part), 4)
    return {
        "voltage": draw_voltage(jax.random.fold_in(jax.random.fold_in(key_of[3], part), 71), part),
        "delays": draw_delays(jax.random.fold_in(key_of[3], 71), part),
        "chan_mask": plant((jax.random.randint(part_splits[2], (NCHAN,), 0, 8) < 7).astype(jnp.int32), jax.random.fold_in(part_splits[2], 1), 0, 1),
    }


def prototype(tap_count, chan_count):
    length = tap_count * chan_count
    position = jnp.arange(length, dtype=jnp.float32)
    centred = (position - (length - 1) / 2.0) / chan_count
    window = 0.54 - 0.46 * jnp.cos(2.0 * jnp.pi * position / (length - 1))
    shaped = jnp.sinc(centred) * window
    shaped = shaped * jnp.sqrt(chan_count / jnp.sum(shaped * shaped))
    return shaped.reshape(tap_count, chan_count)

def dedisperse(padded, delays, out_width, block_rows):
    chan_count = padded.shape[0]
    offsets = jnp.arange(out_width, dtype=jnp.int32)

    def pick_row(row_values, row_delays):
        return row_values[row_delays[:, None] + offsets[None, :]]

    def add_block(block_index, running):
        first_row = (block_index * block_rows).astype(jnp.int32)
        rows_here = lax.dynamic_slice_in_dim(padded, first_row, block_rows, 0)
        delay_here = lax.dynamic_slice_in_dim(delays, first_row, block_rows, 1)
        picked = jax.vmap(pick_row)(rows_here, delay_here.T)
        return running + lax.optimization_barrier(jnp.sum(picked.astype(jnp.float32), axis=0))
    zero_sums = jnp.zeros((delays.shape[0], out_width), jnp.float32)
    return lax.fori_loop(0, chan_count // block_rows, add_block, zero_sums)

def reference(voltage, delays, chan_mask):
    frame_count = voltage.shape[2] // NCHAN
    framed = voltage.astype(jnp.float32).reshape(2, 2, frame_count, NCHAN)
    history = jnp.zeros((2, 2, TAPS - 1, NCHAN), jnp.float32)
    extended = jnp.concatenate([history, framed], axis=2)
    coeffs = prototype(TAPS, NCHAN)
    weighted = jnp.zeros((2, 2, frame_count, NCHAN), jnp.float32)
    for tap_index in range(TAPS):
        weighted = weighted + coeffs[tap_index] * extended[:, :, tap_index:tap_index + frame_count]
    spectra = jnp.fft.fft(lax.complex(weighted[:, 0], weighted[:, 1]), axis=-1) / jnp.sqrt(jnp.float32(NCHAN))
    energy = lax.optimization_barrier(jnp.sum(jnp.real(spectra) ** 2 + jnp.imag(spectra) ** 2, axis=0))
    detected = energy.T.astype(jnp.bfloat16)
    masked = detected * chan_mask.astype(jnp.bfloat16)[:, None]
    padded = jnp.concatenate([masked, jnp.zeros((NCHAN, MAXD), jnp.bfloat16)], axis=1)
    series = dedisperse(padded, delays, frame_count, 16)
    average = lax.optimization_barrier(jnp.sum(series, axis=1)) / frame_count
    peak_value = lax.optimization_barrier(jnp.max(series, axis=1))
    centred = series - average[:, None]
    variance = lax.optimization_barrier(jnp.sum(centred * centred, axis=1)) / frame_count
    deviation = jnp.sqrt(variance + 1e-05)
    zscore = centred / deviation[:, None]
    live_count = jnp.maximum(jnp.sum(chan_mask).astype(jnp.float32), 1.0)
    trial_stats = jnp.stack([average / live_count, deviation / live_count, (peak_value - average) / deviation])
    return (zscore, trial_stats)
```

```python
import math

import jax
import jax.numpy as jnp
from jax import lax
from jax.sharding import PartitionSpec as P

NCHAN = 2048
TAPS = 16
DSPAN = 3


highest = lax.Precision.HIGHEST
shift_group = 8


def passed_along(value, axis, steps):
    count = lax.axis_size(axis)
    first, last = (max(0, -steps), min(count, count - steps))
    return lax.ppermute(value, axis, [(source, source + steps) for source in range(first, last)])


def prototype(tap_count, chan_count):
    length = tap_count * chan_count
    position = jnp.arange(length, dtype=jnp.float32)
    centred = (position - (length - 1) / 2.0) / chan_count
    window = 0.54 - 0.46 * jnp.cos(2.0 * jnp.pi * position / (length - 1))
    shaped = jnp.sinc(centred) * window
    shaped = shaped * jnp.sqrt(chan_count / jnp.sum(shaped * shaped))
    return shaped.reshape(tap_count, chan_count)


def phase_table(row_count, col_count, period):
    product = (
        jnp.arange(row_count, dtype=jnp.int32)[:, None]
        * jnp.arange(col_count, dtype=jnp.int32)[None, :]
        % period
    )
    angles = product.astype(jnp.float32) * (-2.0 * jnp.pi / period)
    return (jnp.cos(angles), jnp.sin(angles))


def spectral_power(weighted, chan_count):
    frame_count = weighted.shape[2]
    low_count = chan_count // 128
    split_up = weighted.reshape(2, 2, frame_count, low_count, 128)
    real_part = split_up[:, 0]
    imag_part = split_up[:, 1]
    cos_first, sin_first = phase_table(low_count, low_count, low_count)
    section_real = jnp.einsum(
        "pfmn,mk->pfkn", real_part, cos_first, precision=highest
    ) - jnp.einsum("pfmn,mk->pfkn", imag_part, sin_first, precision=highest)
    section_imag = jnp.einsum(
        "pfmn,mk->pfkn", real_part, sin_first, precision=highest
    ) + jnp.einsum("pfmn,mk->pfkn", imag_part, cos_first, precision=highest)
    cos_twist, sin_twist = phase_table(low_count, 128, chan_count)
    twist_real = section_real * cos_twist - section_imag * sin_twist
    twist_imag = section_real * sin_twist + section_imag * cos_twist
    cos_second, sin_second = phase_table(128, 128, 128)
    scale_factor = 1.0 / math.sqrt(chan_count)
    cos_second = cos_second * scale_factor
    sin_second = sin_second * scale_factor
    final_real = jnp.einsum(
        "pfkn,nj->pfkj", twist_real, cos_second, precision=highest
    ) - jnp.einsum("pfkn,nj->pfkj", twist_imag, sin_second, precision=highest)
    final_imag = jnp.einsum(
        "pfkn,nj->pfkj", twist_real, sin_second, precision=highest
    ) + jnp.einsum("pfkn,nj->pfkj", twist_imag, cos_second, precision=highest)
    energy = jnp.sum(final_real * final_real + final_imag * final_imag, axis=0)
    return jnp.transpose(energy, (2, 1, 0)).reshape(chan_count, frame_count).astype(jnp.bfloat16)


def dedisperse(padded, delays, out_width, max_delay):
    chan_count = padded.shape[0]
    group_count = (max_delay + shift_group) // shift_group
    needed = out_width + group_count * shift_group
    padded = jnp.concatenate(
        [padded, jnp.zeros((chan_count, needed - padded.shape[1]), padded.dtype)], axis=1
    )
    within = jnp.arange(shift_group, dtype=jnp.int32)

    def add_group(group_index, running):
        base = (group_index * shift_group).astype(jnp.int32)
        window = lax.dynamic_slice_in_dim(padded, base, out_width + shift_group - 1, 1)
        stacked = jnp.stack(
            [window[:, offset : offset + out_width] for offset in range(shift_group)]
        )
        targets = base + within
        selector = (delays[:, None, :] == targets[None, :, None]).astype(jnp.bfloat16)
        return running + jnp.einsum(
            "dsk,skt->dt", selector, stacked, preferred_element_type=jnp.float32
        )

    zero_sums = jnp.zeros((delays.shape[0], out_width), jnp.float32)
    return lax.fori_loop(0, group_count, add_group, zero_sums)


def per_device(voltage, delays, chan_mask):
    frame_count = voltage.shape[2] // NCHAN
    framed = voltage.reshape(2, 2, frame_count, NCHAN)
    history = passed_along(framed[:, :, frame_count - (TAPS - 1) :], "tm", 1)
    extended = jnp.concatenate([history, framed], axis=2)
    coeffs = prototype(TAPS, NCHAN)
    weighted = jnp.zeros((2, 2, frame_count, NCHAN), jnp.float32)
    for tap_index in range(TAPS):
        weighted = weighted + coeffs[tap_index] * extended[
            :, :, tap_index : tap_index + frame_count
        ].astype(jnp.float32)
    detected = spectral_power(weighted, NCHAN)
    masked = detected * chan_mask.astype(jnp.bfloat16)[:, None]
    max_delay = DSPAN * frame_count
    gathered = masked
    held_shards = 1
    while held_shards < DSPAN + 1:
        fetched = passed_along(gathered, "tm", -held_shards)
        gathered = jnp.concatenate([gathered, fetched], axis=1)
        held_shards = held_shards * 2
    series = dedisperse(gathered, delays, frame_count, max_delay)
    local_frames = series.shape[1]
    total_frames = local_frames * lax.axis_size("tm")
    local_sum = jnp.sum(series, axis=1)
    local_centred = series - (local_sum / local_frames)[:, None]
    packed = jnp.stack(
        [local_sum, jnp.max(series, axis=1), jnp.sum(local_centred * local_centred, axis=1)]
    )
    count = lax.axis_size("tm")
    shared = lax.all_to_all(jnp.broadcast_to(packed[None], (count,) + packed.shape), "tm", 0, 0)
    average = jnp.sum(shared[:, 0], axis=0) / total_frames
    peak_value = jnp.max(shared[:, 1], axis=0)
    drift = shared[:, 0] / local_frames - average
    variance = jnp.sum(shared[:, 2] + local_frames * drift * drift, axis=0) / total_frames
    centred = series - average[:, None]
    deviation = jnp.sqrt(variance + 1e-05)
    zscore = centred / deviation[:, None]
    live_count = jnp.maximum(jnp.sum(chan_mask).astype(jnp.float32), 1.0)
    trial_stats = jnp.stack(
        [average / live_count, deviation / live_count, (peak_value - average) / deviation]
    )
    return (zscore, trial_stats)


def solution(mesh):
    in_specs = (P(None, None, ("beam", "tm")), P(), P("beam"))
    out_specs = (P(None, ("beam", "tm")), P(None, "beam"))
    return jax.shard_map(
        per_device, mesh=mesh, in_specs=in_specs, out_specs=out_specs, check_vma=False
    )
```

```python
import math

import jax
import jax.numpy as jnp
import numpy as np
from jax import lax
from jax.experimental import pallas as pl
from jax.experimental.pallas import tpu as pltpu
from jax.sharding import PartitionSpec as P

NCHAN = 2048
TAPS = 16
DSPAN = 3
LANES = 128
RADIX = NCHAN // LANES
GROUP = 8
TILE = 256
NTILE = NCHAN // TILE
CHUNK = 4

f32 = jnp.float32
bf16 = jnp.bfloat16


def split_pair(table):
    table = np.asarray(table, np.float32)
    high = table.astype(jnp.bfloat16)
    low = (table - high.astype(np.float32)).astype(jnp.bfloat16)
    return np.stack([high, low])


def make_tables():
    length = TAPS * NCHAN
    position = np.arange(length, dtype=np.float64)
    window = 0.54 - 0.46 * np.cos(2.0 * np.pi * position / (length - 1))
    shaped = np.sinc((position - (length - 1) / 2.0) / NCHAN) * window
    shaped = shaped * np.sqrt(NCHAN / np.sum(shaped * shaped))
    coeffs = shaped.reshape(TAPS * RADIX, LANES).astype(np.float32)
    rows = np.arange(RADIX)
    angle = 2.0 * np.pi * np.outer(rows, rows) / RADIX
    eye = np.eye(GROUP)
    cos_one, sin_one = np.kron(eye, np.cos(angle)), np.kron(eye, np.sin(angle))
    first = split_pair(np.block([[cos_one, sin_one], [-sin_one, cos_one]]))
    lanes = np.arange(LANES)
    angle = 2.0 * np.pi * np.outer(rows, lanes) / NCHAN
    twist = np.stack([np.tile(np.cos(angle), (GROUP, 1)), np.tile(np.sin(angle), (GROUP, 1))])
    angle = 2.0 * np.pi * np.outer(lanes, lanes) / LANES
    scale = 1.0 / math.sqrt(NCHAN)
    cos_two, sin_two = scale * np.cos(angle), scale * np.sin(angle)
    second = split_pair(np.block([[cos_two, -sin_two], [sin_two, cos_two]]))
    low_count = TILE // RADIX
    order = np.zeros((TILE, TILE), np.float32)
    for k_one in range(RADIX):
        for k_low in range(low_count):
            order[k_low * RADIX + k_one, k_one * low_count + k_low] = 1.0
    return coeffs, first, twist.astype(np.float32), second, order.astype(jnp.bfloat16)


def halves(value):
    high = value.astype(bf16)
    return high, (value - high.astype(f32)).astype(bf16)


def dot(left, right):
    return jnp.dot(left, right, preferred_element_type=f32)


def roll_left(value, steps):
    width = value.shape[-1]
    return pltpu.roll(value, (width - steps) % width, axis=value.ndim - 1)


def prep_kernel(delays_ref, mask_ref, order_ref, rel_ref, base_ref, reach_ref):
    order = order_ref[...]
    for tile in range(NTILE):
        here = delays_ref[:, tile * TILE : (tile + 1) * TILE]
        least = here[:, TILE - 1 : TILE]
        live = mask_ref[:, tile * TILE : (tile + 1) * TILE] > 0
        rel = jnp.where(live, here - least, -1).astype(f32).astype(bf16)
        rel_ref[:, tile * TILE : (tile + 1) * TILE] = dot(rel, order)
        base_ref[tile] = jnp.broadcast_to(least, base_ref.shape[1:])
        reach_ref[tile] = jnp.max(here[:, 0:1] - least)


def main_kernel(reach_ref, x_ref, hist_ref, coeffs_ref, first_ref, twist_ref, second_ref, rel_ref,
                base_ref, out_ref, ext_ref, weighted_ref, det_ref, tile_ref, acc_ref):
    frames = x_ref.shape[1] // RADIX
    past = (TAPS - 1) * RADIX
    for plane in range(4):
        ext_ref[plane, :past] = hist_ref[plane].astype(f32)
        ext_ref[plane, past:] = x_ref[plane].astype(f32)
    tile_ref[...] = jnp.zeros_like(tile_ref)

    for half in range(RADIX // 8):
        taps = [coeffs_ref[tap * RADIX + half * 8 : tap * RADIX + half * 8 + 8] for tap in range(TAPS)]

        def weigh(group, carry):
            for plane in range(4):
                pol, part = divmod(plane, 2)
                for inner in range(GROUP):
                    start = pl.multiple_of((group * GROUP + inner) * RADIX + half * 8, 8)
                    total = None
                    for tap in range(TAPS):
                        term = taps[tap] * ext_ref[plane, pl.ds(start + tap * RADIX, 8)]
                        total = term if total is None else total + term
                    row = part * GROUP * RADIX + inner * RADIX + half * 8
                    weighted_ref[group, row : row + 8, pol * LANES : (pol + 1) * LANES] = total
            return carry

        lax.fori_loop(0, frames // GROUP, weigh, 0)

    span = GROUP * RADIX
    twist_cos, twist_sin = twist_ref[0], twist_ref[1]
    for group in range(frames // GROUP):
        high, low = halves(weighted_ref[group])
        mixed = dot(first_ref[0], high) + dot(first_ref[0], low) + dot(first_ref[1], high)
        energy = None
        for pol in range(2):
            real = mixed[:span, pol * LANES : (pol + 1) * LANES]
            imag = mixed[span:, pol * LANES : (pol + 1) * LANES]
            turned = jnp.concatenate(
                [real * twist_cos + imag * twist_sin, imag * twist_cos - real * twist_sin], axis=1
            )
            high, low = halves(turned)
            final = dot(high, second_ref[0]) + dot(low, second_ref[0]) + dot(high, second_ref[1])
            square = final * final
            power = square[:, :LANES] + square[:, LANES:]
            energy = power if energy is None else energy + power
        det_ref[group * span : (group + 1) * span] = energy.astype(bf16).astype(f32)

    width = LANES // 8
    lane_group = lax.broadcasted_iota(jnp.int32, (frames, LANES), 1) // width
    for half in range(RADIX // 8):
        rows = [det_ref[pl.ds(half * 8 + index, frames, stride=RADIX), :] for index in range(8)]
        for bit in (4, 2, 1):
            upper = (lane_group & bit) != 0
            for index in range(8):
                if index & bit:
                    continue
                one, two = rows[index], rows[index + bit]
                rows[index] = jnp.where(upper, pltpu.roll(two, bit * width, axis=1), one)
                rows[index + bit] = jnp.where(upper, two, roll_left(one, bit * width))
        for tile in range(NTILE):
            tile_ref[tile, DSPAN * frames :, half * LANES : (half + 1) * LANES] = rows[tile].astype(bf16)

    trials = rel_ref.shape[0]
    acc_ref[...] = jnp.zeros_like(acc_ref)
    most = reach_ref[0]
    for tile in range(1, NTILE):
        most = jnp.maximum(most, reach_ref[tile])
    steps = most // CHUNK + 1

    def add_chunk(step, carry):
        lowest = (steps - 1 - step) * CHUNK
        for tile in range(NTILE):
            rel = rel_ref[:, tile * TILE : (tile + 1) * TILE]
            chosen = jnp.concatenate(
                [
                    jnp.where(rel == (lowest + offset).astype(f32), 1.0, 0.0).astype(bf16)
                    for offset in range(CHUNK)
                ],
                axis=0,
            )
            sums = lax.dot_general(
                chosen, tile_ref[tile], (((1,), (1,)), ((), ())), preferred_element_type=f32
            )
            acc = acc_ref[tile]
            for offset in reversed(range(CHUNK)):
                acc = roll_left(acc, 1) + sums[offset * trials : (offset + 1) * trials]
            acc_ref[tile] = acc
        return carry

    lax.fori_loop(0, steps, add_chunk, 0)

    total = None
    for tile in range(NTILE):
        base = base_ref[tile]
        value = acc_ref[tile]
        bit = 1
        while bit <= DSPAN * frames:
            value = jnp.where((base & bit) != 0, roll_left(value, bit), value)
            bit *= 2
        total = value if total is None else total + value
    out_ref[...] = total


def stats_kernel(where_ref, parts_ref, mask_ref, zscore_ref, stats_ref):
    count, trials, width = parts_ref.shape
    frames = zscore_ref.shape[1]
    share = width // frames
    lane = lax.broadcasted_iota(jnp.int32, (trials, width), 1)
    block = lane // frames
    sums = [None] * (count // share)

    def put(index, value):
        sums[index] = value if sums[index] is None else sums[index] + value

    for device in range(count):
        part = parts_ref[device]
        turn = frames * ((device + 1) % share)
        if turn:
            part = pltpu.roll(part, turn, axis=1)
        group, within = divmod(device, share)
        stays = block <= within
        put(group, jnp.where(stays, part, 0.0))
        if group > 0 and within < share - 1:
            put(group - 1, jnp.where(stays, 0.0, part))
    total_frames = float(count * frames)
    whole, peak = sums[0], sums[0]
    for part in sums[1:]:
        whole = whole + part
        peak = jnp.maximum(peak, part)
    average = jnp.sum(whole, axis=1, keepdims=True) / total_frames
    peak_value = jnp.max(peak, axis=1, keepdims=True)
    squares = None
    mine = jnp.zeros((trials, width), f32)
    own_group = where_ref[0] // share
    for index, part in enumerate(sums):
        centred = part - average
        square = centred * centred
        squares = square if squares is None else squares + square
        mine = jnp.where(own_group == index, centred, mine)
    variance = jnp.sum(squares, axis=1, keepdims=True) / total_frames
    deviation = jnp.sqrt(variance + 1e-05)
    own_block = where_ref[0] % share
    picked = None
    for index in range(share):
        piece = jnp.where(own_block == index, mine[:, index * frames : (index + 1) * frames], 0.0)
        picked = piece if picked is None else picked + piece
    zscore_ref[...] = picked / deviation
    live = jnp.sum(mask_ref[...].astype(f32), axis=1, keepdims=True)
    live = jnp.maximum(live, 1.0)
    row = lax.broadcasted_iota(jnp.int32, (trials, width), 0)
    for index, column in enumerate((average / live, deviation / live, (peak_value - average) / deviation)):
        spread = jnp.where(row == lane, column, 0.0)
        stats_ref[index : index + 1, :] = jnp.sum(spread, axis=0, keepdims=True)[:, :trials]


def per_device(voltage, delays, chan_mask):
    frames = voltage.shape[2] // NCHAN
    trials = delays.shape[0]
    coeffs, first, twist, second, order = make_tables()
    framed = voltage.reshape(4, frames * RADIX, LANES)
    count = lax.axis_size("tm")
    hist = lax.ppermute(
        framed[:, (frames - TAPS + 1) * RADIX :], "tm", [(i, i + 1) for i in range(count - 1)]
    )
    mask_row = chan_mask.reshape(1, NCHAN)
    vmem = pl.BlockSpec(memory_space=pltpu.VMEM)
    smem = pl.BlockSpec(memory_space=pltpu.SMEM)
    rel, base, reach = pl.pallas_call(
        prep_kernel,
        name="prep",
        out_shape=(
            jax.ShapeDtypeStruct((trials, NCHAN), f32),
            jax.ShapeDtypeStruct((NTILE, trials, LANES), jnp.int32),
            jax.ShapeDtypeStruct((NTILE,), jnp.int32),
        ),
        in_specs=[vmem] * 3,
        out_specs=(vmem, vmem, smem),
    )(delays, mask_row, order)
    window = (DSPAN + 1) * frames
    partial = pl.pallas_call(
        main_kernel,
        name="channelize",
        out_shape=jax.ShapeDtypeStruct((trials, window), f32),
        in_specs=[smem] + [vmem] * 8,
        out_specs=vmem,
        scratch_shapes=[
            pltpu.VMEM((4, (frames + TAPS - 1) * RADIX, LANES), f32),
            pltpu.VMEM((frames // GROUP, 2 * GROUP * RADIX, 2 * LANES), f32),
            pltpu.VMEM((frames * RADIX, LANES), f32),
            pltpu.VMEM((NTILE, window, TILE), bf16),
            pltpu.VMEM((NTILE, trials, window), f32),
        ],
    )(reach, framed, hist, coeffs, first, twist, second, rel, base)
    parts = lax.all_to_all(jnp.broadcast_to(partial[None], (count, trials, window)), "tm", 0, 0)
    here = lax.axis_index("tm").astype(jnp.int32).reshape(1)
    return pl.pallas_call(
        stats_kernel,
        name="normalize",
        out_shape=(
            jax.ShapeDtypeStruct((trials, frames), f32),
            jax.ShapeDtypeStruct((3, trials), f32),
        ),
        in_specs=[smem, vmem, vmem],
        out_specs=(vmem, vmem),
    )(here, parts, mask_row)


def solution(mesh):
    in_specs = (P(None, None, ("beam", "tm")), P(), P("beam"))
    out_specs = (P(None, ("beam", "tm")), P(None, "beam"))
    return jax.shard_map(
        per_device, mesh=mesh, in_specs=in_specs, out_specs=out_specs, check_vma=False
    )
```

```python
import math

import jax
import jax.numpy as jnp
import numpy as np
from jax import lax
from jax.experimental import pallas as pl
from jax.experimental.pallas import tpu as pltpu
from jax.sharding import PartitionSpec as P

NCHAN = 2048
TAPS = 16
DSPAN = 3
LANES = 128
RADIX = NCHAN // LANES
GROUP = 8
TILE = 256
NTILE = NCHAN // TILE
CHUNK = 6
GRANT = 16 * 1024 * 1024

f32 = jnp.float32
bf16 = jnp.bfloat16


def split_pair(table):
    table = np.asarray(table, np.float32)
    high = table.astype(jnp.bfloat16)
    low = (table - high.astype(np.float32)).astype(jnp.bfloat16)
    return np.stack([high, low])


def make_tables():
    length = TAPS * NCHAN
    position = np.arange(length, dtype=np.float64)
    window = 0.54 - 0.46 * np.cos(2.0 * np.pi * position / (length - 1))
    shaped = np.sinc((position - (length - 1) / 2.0) / NCHAN) * window
    shaped = shaped * np.sqrt(NCHAN / np.sum(shaped * shaped))
    coeffs = shaped.reshape(TAPS * RADIX, LANES).astype(np.float32)
    rows = np.arange(RADIX)
    angle = 2.0 * np.pi * np.outer(rows, rows) / RADIX
    eye = np.eye(GROUP)
    cos_one, sin_one = np.kron(eye, np.cos(angle)), np.kron(eye, np.sin(angle))
    first = split_pair(np.block([[cos_one, sin_one], [-sin_one, cos_one]]))
    lanes = np.arange(LANES)
    angle = 2.0 * np.pi * np.outer(rows, lanes) / NCHAN
    twist = np.stack([np.tile(np.cos(angle), (GROUP, 1)), np.tile(np.sin(angle), (GROUP, 1))])
    angle = 2.0 * np.pi * np.outer(lanes, lanes) / LANES
    scale = 1.0 / math.sqrt(NCHAN)
    cos_two, sin_two = scale * np.cos(angle), scale * np.sin(angle)
    second = split_pair(np.block([[cos_two, -sin_two], [sin_two, cos_two]]))
    low_count = TILE // RADIX
    order = np.zeros((TILE, TILE), np.float32)
    for k_one in range(RADIX):
        for k_low in range(low_count):
            order[k_low * RADIX + k_one, k_one * low_count + k_low] = 1.0
    return coeffs, first, twist.astype(np.float32), second, order.astype(jnp.bfloat16)


def halves(value):
    high = value.astype(bf16)
    return high, (value - high.astype(f32)).astype(bf16)


def dot(left, right):
    return jnp.dot(left, right, preferred_element_type=f32)


def roll_left(value, steps):
    width = value.shape[-1]
    return pltpu.roll(value, (width - steps) % width, axis=value.ndim - 1)


def prep_kernel(delays_ref, mask_ref, order_ref, rel_ref, base_ref, reach_ref):
    order = order_ref[...]
    for tile in range(NTILE):
        here = delays_ref[:, tile * TILE : (tile + 1) * TILE]
        least = here[:, TILE - 1 : TILE]
        live = mask_ref[:, tile * TILE : (tile + 1) * TILE] > 0
        rel = jnp.where(live, here - least, -1).astype(f32).astype(bf16)
        rel_ref[:, tile * TILE : (tile + 1) * TILE] = dot(rel, order).astype(bf16)
        base_ref[tile] = jnp.broadcast_to(least, base_ref.shape[1:])
        reach_ref[tile] = jnp.max(here[:, 0:1] - least)


def main_kernel(reach_ref, x_ref, hist_ref, coeffs_ref, first_ref, twist_ref, second_ref, rel_ref,
                base_ref, out_ref, ext_ref, weighted_ref, det_ref, tile_ref, acc_ref):
    frames = x_ref.shape[1] // RADIX
    past = (TAPS - 1) * RADIX
    for plane in range(4):
        ext_ref[plane, :past] = hist_ref[plane].astype(f32)
        ext_ref[plane, past:] = x_ref[plane].astype(f32)
    tile_ref[...] = jnp.zeros_like(tile_ref)

    for half in range(RADIX // 8):
        taps = [coeffs_ref[tap * RADIX + half * 8 : tap * RADIX + half * 8 + 8] for tap in range(TAPS)]

        def weigh(group, carry):
            for plane in range(4):
                pol, part = divmod(plane, 2)
                for inner in range(GROUP):
                    start = pl.multiple_of((group * GROUP + inner) * RADIX + half * 8, 8)
                    total = None
                    for tap in range(TAPS):
                        term = taps[tap] * ext_ref[plane, pl.ds(start + tap * RADIX, 8)]
                        total = term if total is None else total + term
                    row = part * GROUP * RADIX + inner * RADIX + half * 8
                    weighted_ref[group, row : row + 8, pol * LANES : (pol + 1) * LANES] = total
            return carry

        lax.fori_loop(0, frames // GROUP, weigh, 0)

    span = GROUP * RADIX
    twist_cos, twist_sin = twist_ref[0], twist_ref[1]
    for group in range(frames // GROUP):
        high, low = halves(weighted_ref[group])
        mixed = dot(first_ref[0], high) + dot(first_ref[0], low) + dot(first_ref[1], high)
        energy = None
        for pol in range(2):
            real = mixed[:span, pol * LANES : (pol + 1) * LANES]
            imag = mixed[span:, pol * LANES : (pol + 1) * LANES]
            turned = jnp.concatenate(
                [real * twist_cos + imag * twist_sin, imag * twist_cos - real * twist_sin], axis=1
            )
            high, low = halves(turned)
            final = dot(high, second_ref[0]) + dot(low, second_ref[0]) + dot(high, second_ref[1])
            square = final * final
            power = square[:, :LANES] + square[:, LANES:]
            energy = power if energy is None else energy + power
        det_ref[group * span : (group + 1) * span] = energy.astype(bf16).astype(f32)

    width = LANES // 8
    lane_group = lax.broadcasted_iota(jnp.int32, (frames, LANES), 1) // width
    for half in range(RADIX // 8):
        rows = [det_ref[pl.ds(half * 8 + index, frames, stride=RADIX), :] for index in range(8)]
        for bit in (4, 2, 1):
            upper = (lane_group & bit) != 0
            for index in range(8):
                if index & bit:
                    continue
                one, two = rows[index], rows[index + bit]
                rows[index] = jnp.where(upper, pltpu.roll(two, bit * width, axis=1), one)
                rows[index + bit] = jnp.where(upper, two, roll_left(one, bit * width))
        for tile in range(NTILE):
            tile_ref[tile, DSPAN * frames :, half * LANES : (half + 1) * LANES] = rows[tile].astype(bf16)

    trials = rel_ref.shape[0]
    acc_ref[...] = jnp.zeros_like(acc_ref)
    most = reach_ref[0]
    for tile in range(1, NTILE):
        most = jnp.maximum(most, reach_ref[tile])
    steps = most // CHUNK + 1
    one = jnp.ones((trials, TILE), bf16)
    zero = jnp.zeros((trials, TILE), bf16)

    def add_chunk(step, carry):
        lowest = (steps - 1 - step) * CHUNK
        for tile in range(NTILE):
            rel = rel_ref[:, tile * TILE : (tile + 1) * TILE]
            chosen = jnp.concatenate(
                [
                    jnp.where(rel == (lowest + offset).astype(f32).astype(bf16), one, zero)
                    for offset in range(CHUNK)
                ],
                axis=0,
            )
            sums = lax.dot_general(
                chosen, tile_ref[tile], (((1,), (1,)), ((), ())), preferred_element_type=f32
            )
            acc = acc_ref[tile]
            for offset in reversed(range(CHUNK)):
                acc = roll_left(acc, 1) + sums[offset * trials : (offset + 1) * trials]
            acc_ref[tile] = acc
        return carry

    lax.fori_loop(0, steps, add_chunk, 0)

    total = None
    for tile in range(NTILE):
        base = base_ref[tile]
        value = acc_ref[tile]
        bit = 1
        while bit <= DSPAN * frames:
            value = jnp.where((base & bit) != 0, roll_left(value, bit), value)
            bit *= 2
        total = value if total is None else total + value
    for device in range(out_ref.shape[0]):
        out_ref[device] = total


def stats_kernel(where_ref, parts_ref, mask_ref, zscore_ref, stats_ref):
    count, trials, width = parts_ref.shape
    frames = zscore_ref.shape[0]
    share = width // frames
    lane = lax.broadcasted_iota(jnp.int32, (trials, width), 1)
    block = lane // frames
    sums = [None] * (count // share)

    def put(index, value):
        sums[index] = value if sums[index] is None else sums[index] + value

    for device in range(count):
        part = parts_ref[device]
        turn = frames * ((device + 1) % share)
        if turn:
            part = pltpu.roll(part, turn, axis=1)
        group, within = divmod(device, share)
        stays = block <= within
        put(group, jnp.where(stays, part, 0.0))
        if group > 0 and within < share - 1:
            put(group - 1, jnp.where(stays, 0.0, part))
    total_frames = float(count * frames)
    whole, peak = sums[0], sums[0]
    for part in sums[1:]:
        whole = whole + part
        peak = jnp.maximum(peak, part)
    average = jnp.sum(whole, axis=1, keepdims=True) / total_frames
    peak_value = jnp.max(peak, axis=1, keepdims=True)
    squares = None
    mine = jnp.zeros((trials, width), f32)
    own_group = where_ref[0] // share
    for index, part in enumerate(sums):
        centred = part - average
        square = centred * centred
        squares = square if squares is None else squares + square
        mine = jnp.where(own_group == index, centred, mine)
    variance = jnp.sum(squares, axis=1, keepdims=True) / total_frames
    deviation = jnp.sqrt(variance + 1e-05)
    own_block = where_ref[0] % share
    scaled = (mine / deviation).T
    picked = None
    for index in range(share):
        piece = jnp.where(own_block == index, scaled[index * frames : (index + 1) * frames], 0.0)
        picked = piece if picked is None else picked + piece
    zscore_ref[...] = picked
    live = jnp.sum(mask_ref[...].astype(f32), axis=1, keepdims=True)
    live = jnp.maximum(live, 1.0)
    row = lax.broadcasted_iota(jnp.int32, (trials, width), 0)
    for index, column in enumerate((average / live, deviation / live, (peak_value - average) / deviation)):
        spread = jnp.where(row == lane, column, 0.0)
        stats_ref[index : index + 1, :] = jnp.sum(spread, axis=0, keepdims=True)[:, :trials]


def per_device(voltage, delays, chan_mask):
    frames = voltage.shape[2] // NCHAN
    trials = delays.shape[0]
    coeffs, first, twist, second, order = make_tables()
    framed = voltage.reshape(4, frames * RADIX, LANES)
    count = lax.axis_size("tm")
    hist = lax.ppermute(
        framed[:, (frames - TAPS + 1) * RADIX :], "tm", [(i, i + 1) for i in range(count - 1)]
    )
    mask_row = chan_mask.reshape(1, NCHAN)
    vmem = pl.BlockSpec(memory_space=pltpu.VMEM)
    smem = pl.BlockSpec(memory_space=pltpu.SMEM)
    rel, base, reach = pl.pallas_call(
        prep_kernel,
        name="prep",
        compiler_params=pltpu.CompilerParams(vmem_limit_bytes=GRANT),
        out_shape=(
            jax.ShapeDtypeStruct((trials, NCHAN), bf16),
            jax.ShapeDtypeStruct((NTILE, trials, LANES), jnp.int32),
            jax.ShapeDtypeStruct((NTILE,), jnp.int32),
        ),
        in_specs=[vmem] * 3,
        out_specs=(vmem, vmem, smem),
    )(delays, mask_row, order)
    window = (DSPAN + 1) * frames
    partial = pl.pallas_call(
        main_kernel,
        name="channelize",
        compiler_params=pltpu.CompilerParams(vmem_limit_bytes=GRANT),
        out_shape=jax.ShapeDtypeStruct((count, trials, window), f32),
        in_specs=[smem] + [vmem] * 8,
        out_specs=vmem,
        scratch_shapes=[
            pltpu.VMEM((4, (frames + TAPS - 1) * RADIX, LANES), f32),
            pltpu.VMEM((frames // GROUP, 2 * GROUP * RADIX, 2 * LANES), f32),
            pltpu.VMEM((frames * RADIX, LANES), f32),
            pltpu.VMEM((NTILE, window, TILE), bf16),
            pltpu.VMEM((NTILE, trials, window), f32),
        ],
    )(reach, framed, hist, coeffs, first, twist, second, rel, base)
    parts = lax.all_to_all(partial, "tm", 0, 0)
    here = lax.axis_index("tm").astype(jnp.int32).reshape(1)
    zscore, trial_stats = pl.pallas_call(
        stats_kernel,
        name="normalize",
        compiler_params=pltpu.CompilerParams(vmem_limit_bytes=GRANT),
        out_shape=(
            jax.ShapeDtypeStruct((frames, trials), f32),
            jax.ShapeDtypeStruct((3, trials), f32),
        ),
        in_specs=[smem, vmem, vmem],
        out_specs=(vmem, vmem),
    )(here, parts, mask_row)
    return zscore.T, trial_stats


def solution(mesh):
    in_specs = (P(None, None, ("beam", "tm")), P(), P("beam"))
    out_specs = (P(None, ("beam", "tm")), P(None, "beam"))
    return jax.shard_map(
        per_device, mesh=mesh, in_specs=in_specs, out_specs=out_specs, check_vma=False
    )
```

```python
import math

import jax
import jax.numpy as jnp
import numpy as np
from jax import lax
from jax.experimental import pallas as pl
from jax.experimental.pallas import tpu as pltpu
from jax.sharding import PartitionSpec as P

NCHAN = 2048
TAPS = 16
DSPAN = 3
LANES = 128
RADIX = NCHAN // LANES
GROUP = 8
TILE = 256
NTILE = NCHAN // TILE
CHUNK = 6
GRANT = 16 * 1024 * 1024

f32 = jnp.float32
bf16 = jnp.bfloat16


def split_pair(table):
    table = np.asarray(table, np.float32)
    high = table.astype(jnp.bfloat16)
    low = (table - high.astype(np.float32)).astype(jnp.bfloat16)
    return np.stack([high, low])


def make_tables():
    length = TAPS * NCHAN
    position = np.arange(length, dtype=np.float64)
    window = 0.54 - 0.46 * np.cos(2.0 * np.pi * position / (length - 1))
    shaped = np.sinc((position - (length - 1) / 2.0) / NCHAN) * window
    shaped = shaped * np.sqrt(NCHAN / np.sum(shaped * shaped))
    coeffs = shaped.reshape(TAPS * RADIX, LANES).astype(np.float32)
    rows = np.arange(RADIX)
    angle = 2.0 * np.pi * np.outer(rows, rows) / RADIX
    eye = np.eye(GROUP)
    cos_one, sin_one = np.kron(eye, np.cos(angle)), np.kron(eye, np.sin(angle))
    first = split_pair(np.block([[cos_one, sin_one], [-sin_one, cos_one]]))
    lanes = np.arange(LANES)
    angle = 2.0 * np.pi * np.outer(rows, lanes) / NCHAN
    twist = np.stack([np.tile(np.cos(angle), (GROUP, 1)), np.tile(np.sin(angle), (GROUP, 1))])
    angle = 2.0 * np.pi * np.outer(lanes, lanes) / LANES
    scale = 1.0 / math.sqrt(NCHAN)
    cos_two, sin_two = scale * np.cos(angle), scale * np.sin(angle)
    second = split_pair(np.block([[cos_two, -sin_two], [sin_two, cos_two]]))
    low_count = TILE // RADIX
    order = np.zeros((TILE, TILE), np.float32)
    for k_one in range(RADIX):
        for k_low in range(low_count):
            order[k_low * RADIX + k_one, k_one * low_count + k_low] = 1.0
    return coeffs, first, twist.astype(np.float32), second, order.astype(jnp.bfloat16)


def halves(value):
    high = value.astype(bf16)
    return high, (value - high.astype(f32)).astype(bf16)


def dot(left, right):
    return jnp.dot(left, right, preferred_element_type=f32)


def roll_left(value, steps):
    width = value.shape[-1]
    return pltpu.roll(value, (width - steps) % width, axis=value.ndim - 1)


def detect(ext_ref, coeffs_ref, first_ref, twist_ref, second_ref, weighted_ref, det_ref):
    for half in range(RADIX // 8):
        taps = [coeffs_ref[tap * RADIX + half * 8 : tap * RADIX + half * 8 + 8] for tap in range(TAPS)]

        def weigh(group, carry):
            for plane in range(4):
                pol, part = divmod(plane, 2)
                for inner in range(GROUP):
                    start = pl.multiple_of((group * GROUP + inner) * RADIX + half * 8, 8)
                    total = None
                    for tap in range(TAPS):
                        term = taps[tap] * ext_ref[plane, pl.ds(start + tap * RADIX, 8)]
                        total = term if total is None else total + term
                    row = part * GROUP * RADIX + inner * RADIX + half * 8
                    weighted_ref[group, row : row + 8, pol * LANES : (pol + 1) * LANES] = total
            return carry

        lax.fori_loop(0, det_ref.shape[0] // (GROUP * RADIX), weigh, 0)

    span = GROUP * RADIX
    twist_cos, twist_sin = twist_ref[0], twist_ref[1]
    for group in range(det_ref.shape[0] // (GROUP * RADIX)):
        high, low = halves(weighted_ref[group])
        mixed = dot(first_ref[0], high) + dot(first_ref[0], low) + dot(first_ref[1], high)
        energy = None
        for pol in range(2):
            real = mixed[:span, pol * LANES : (pol + 1) * LANES]
            imag = mixed[span:, pol * LANES : (pol + 1) * LANES]
            turned = jnp.concatenate(
                [real * twist_cos + imag * twist_sin, imag * twist_cos - real * twist_sin], axis=1
            )
            high, low = halves(turned)
            final = dot(high, second_ref[0]) + dot(low, second_ref[0]) + dot(high, second_ref[1])
            square = final * final
            power = square[:, :LANES] + square[:, LANES:]
            energy = power if energy is None else energy + power
        det_ref[group * span : (group + 1) * span] = energy.astype(bf16).astype(f32)


def early_kernel(delays_ref, mask_ref, order_ref, x_ref, coeffs_ref, first_ref, twist_ref, second_ref,
                 rel_ref, base_ref, reach_ref, late_ref, ext_ref, weighted_ref):
    start = x_ref.shape[1] - ext_ref.shape[1]
    for plane in range(4):
        ext_ref[plane] = x_ref[plane, start:].astype(f32)
    detect(ext_ref, coeffs_ref, first_ref, twist_ref, second_ref, weighted_ref, late_ref)
    order = order_ref[...]
    for tile in range(NTILE):
        here = delays_ref[:, tile * TILE : (tile + 1) * TILE]
        least = here[:, TILE - 1 : TILE]
        live = mask_ref[:, tile * TILE : (tile + 1) * TILE] > 0
        rel = jnp.where(live, here - least, -1).astype(f32).astype(bf16)
        rel_ref[:, tile * TILE : (tile + 1) * TILE] = dot(rel, order).astype(bf16)
        base_ref[tile] = jnp.broadcast_to(least, base_ref.shape[1:])
        reach_ref[tile] = jnp.max(here[:, 0:1] - least)


def main_kernel(reach_ref, x_ref, hist_ref, coeffs_ref, first_ref, twist_ref, second_ref, rel_ref,
                base_ref, late_ref, out_ref, ext_ref, weighted_ref, first_det_ref, det_ref, tile_ref, acc_ref):
    frames = x_ref.shape[1] // RADIX
    past = (TAPS - 1) * RADIX
    middle = frames // 2 * RADIX
    for plane in range(4):
        ext_ref[plane, :past] = hist_ref[plane].astype(f32)
        ext_ref[plane, past:] = x_ref[plane, :middle].astype(f32)
    tile_ref[...] = jnp.zeros_like(tile_ref)
    detect(ext_ref, coeffs_ref, first_ref, twist_ref, second_ref, weighted_ref, first_det_ref)
    det_ref[:middle] = first_det_ref[...]
    det_ref[middle:] = late_ref[...]

    width = LANES // 8
    lane_group = lax.broadcasted_iota(jnp.int32, (frames, LANES), 1) // width
    for half in range(RADIX // 8):
        rows = [det_ref[pl.ds(half * 8 + index, frames, stride=RADIX), :] for index in range(8)]
        for bit in (4, 2, 1):
            upper = (lane_group & bit) != 0
            for index in range(8):
                if index & bit:
                    continue
                one, two = rows[index], rows[index + bit]
                rows[index] = jnp.where(upper, pltpu.roll(two, bit * width, axis=1), one)
                rows[index + bit] = jnp.where(upper, two, roll_left(one, bit * width))
        for tile in range(NTILE):
            tile_ref[tile, DSPAN * frames :, half * LANES : (half + 1) * LANES] = rows[tile].astype(bf16)

    trials = rel_ref.shape[0]
    acc_ref[...] = jnp.zeros_like(acc_ref)
    most = reach_ref[0]
    for tile in range(1, NTILE):
        most = jnp.maximum(most, reach_ref[tile])
    steps = most // CHUNK + 1
    one = jnp.ones((trials, TILE), bf16)
    zero = jnp.zeros((trials, TILE), bf16)

    def add_chunk(step, carry):
        lowest = (steps - 1 - step) * CHUNK
        for tile in range(NTILE):
            rel = rel_ref[:, tile * TILE : (tile + 1) * TILE]
            chosen = jnp.concatenate(
                [
                    jnp.where(rel == (lowest + offset).astype(f32).astype(bf16), one, zero)
                    for offset in range(CHUNK)
                ],
                axis=0,
            )
            sums = lax.dot_general(
                chosen, tile_ref[tile], (((1,), (1,)), ((), ())), preferred_element_type=f32
            )
            acc = acc_ref[tile]
            for offset in reversed(range(CHUNK)):
                acc = roll_left(acc, 1) + sums[offset * trials : (offset + 1) * trials]
            acc_ref[tile] = acc
        return carry

    lax.fori_loop(0, steps, add_chunk, 0)

    total = None
    for tile in range(NTILE):
        base = base_ref[tile]
        value = acc_ref[tile]
        bit = 1
        while bit <= DSPAN * frames:
            value = jnp.where((base & bit) != 0, roll_left(value, bit), value)
            bit *= 2
        total = value if total is None else total + value
    for device in range(out_ref.shape[0]):
        out_ref[device] = total


def stats_kernel(where_ref, parts_ref, mask_ref, zscore_ref, stats_ref):
    count, trials, width = parts_ref.shape
    frames = zscore_ref.shape[0]
    share = width // frames
    lane = lax.broadcasted_iota(jnp.int32, (trials, width), 1)
    block = lane // frames
    sums = [None] * (count // share)

    def put(index, value):
        sums[index] = value if sums[index] is None else sums[index] + value

    for device in range(count):
        part = parts_ref[device]
        turn = frames * ((device + 1) % share)
        if turn:
            part = pltpu.roll(part, turn, axis=1)
        group, within = divmod(device, share)
        stays = block <= within
        put(group, jnp.where(stays, part, 0.0))
        if group > 0 and within < share - 1:
            put(group - 1, jnp.where(stays, 0.0, part))
    total_frames = float(count * frames)
    whole, peak = sums[0], sums[0]
    for part in sums[1:]:
        whole = whole + part
        peak = jnp.maximum(peak, part)
    average = jnp.sum(whole, axis=1, keepdims=True) / total_frames
    peak_value = jnp.max(peak, axis=1, keepdims=True)
    squares = None
    mine = jnp.zeros((trials, width), f32)
    own_group = where_ref[0] // share
    for index, part in enumerate(sums):
        centred = part - average
        square = centred * centred
        squares = square if squares is None else squares + square
        mine = jnp.where(own_group == index, centred, mine)
    variance = jnp.sum(squares, axis=1, keepdims=True) / total_frames
    deviation = jnp.sqrt(variance + 1e-05)
    own_block = where_ref[0] % share
    scaled = (mine / deviation).T
    picked = None
    for index in range(share):
        piece = jnp.where(own_block == index, scaled[index * frames : (index + 1) * frames], 0.0)
        picked = piece if picked is None else picked + piece
    zscore_ref[...] = picked
    live = jnp.sum(mask_ref[...].astype(f32), axis=1, keepdims=True)
    live = jnp.maximum(live, 1.0)
    row = lax.broadcasted_iota(jnp.int32, (trials, width), 0)
    for index, column in enumerate((average / live, deviation / live, (peak_value - average) / deviation)):
        spread = jnp.where(row == lane, column, 0.0)
        stats_ref[index : index + 1, :] = jnp.sum(spread, axis=0, keepdims=True)[:, :trials]


def per_device(voltage, delays, chan_mask):
    frames = voltage.shape[2] // NCHAN
    trials = delays.shape[0]
    coeffs, first, twist, second, order = make_tables()
    framed = voltage.reshape(4, frames * RADIX, LANES)
    count = lax.axis_size("tm")
    hist = lax.ppermute(
        framed[:, (frames - TAPS + 1) * RADIX :], "tm", [(i, i + 1) for i in range(count - 1)]
    )
    mask_row = chan_mask.reshape(1, NCHAN)
    vmem = pl.BlockSpec(memory_space=pltpu.VMEM)
    smem = pl.BlockSpec(memory_space=pltpu.SMEM)
    half = frames // 2
    rel, base, reach, late = pl.pallas_call(
        early_kernel,
        name="early",
        compiler_params=pltpu.CompilerParams(vmem_limit_bytes=GRANT),
        out_shape=(
            jax.ShapeDtypeStruct((trials, NCHAN), bf16),
            jax.ShapeDtypeStruct((NTILE, trials, LANES), jnp.int32),
            jax.ShapeDtypeStruct((NTILE,), jnp.int32),
            jax.ShapeDtypeStruct((half * RADIX, LANES), f32),
        ),
        in_specs=[vmem] * 8,
        out_specs=(vmem, vmem, smem, vmem),
        scratch_shapes=[
            pltpu.VMEM((4, (half + TAPS - 1) * RADIX, LANES), f32),
            pltpu.VMEM((half // GROUP, 2 * GROUP * RADIX, 2 * LANES), f32),
        ],
    )(delays, mask_row, order, framed, coeffs, first, twist, second)
    window = (DSPAN + 1) * frames
    partial = pl.pallas_call(
        main_kernel,
        name="channelize",
        compiler_params=pltpu.CompilerParams(vmem_limit_bytes=GRANT),
        out_shape=jax.ShapeDtypeStruct((count, trials, window), f32),
        in_specs=[smem] + [vmem] * 9,
        out_specs=vmem,
        scratch_shapes=[
            pltpu.VMEM((4, (half + TAPS - 1) * RADIX, LANES), f32),
            pltpu.VMEM((half // GROUP, 2 * GROUP * RADIX, 2 * LANES), f32),
            pltpu.VMEM((half * RADIX, LANES), f32),
            pltpu.VMEM((frames * RADIX, LANES), f32),
            pltpu.VMEM((NTILE, window, TILE), bf16),
            pltpu.VMEM((NTILE, trials, window), f32),
        ],
    )(reach, framed, hist, coeffs, first, twist, second, rel, base, late)
    parts = lax.all_to_all(partial, "tm", 0, 0)
    here = lax.axis_index("tm").astype(jnp.int32).reshape(1)
    zscore, trial_stats = pl.pallas_call(
        stats_kernel,
        name="normalize",
        compiler_params=pltpu.CompilerParams(vmem_limit_bytes=GRANT),
        out_shape=(
            jax.ShapeDtypeStruct((frames, trials), f32),
            jax.ShapeDtypeStruct((3, trials), f32),
        ),
        in_specs=[smem, vmem, vmem],
        out_specs=(vmem, vmem),
    )(here, parts, mask_row)
    return zscore.T, trial_stats


def solution(mesh):
    in_specs = (P(None, None, ("beam", "tm")), P(), P("beam"))
    out_specs = (P(None, ("beam", "tm")), P(None, "beam"))
    return jax.shard_map(
        per_device, mesh=mesh, in_specs=in_specs, out_specs=out_specs, check_vma=False
    )
```

```python
import math

import jax
import jax.numpy as jnp
import numpy as np
from jax import lax
from jax.experimental import pallas as pl
from jax.experimental.pallas import tpu as pltpu
from jax.sharding import PartitionSpec as P

NCHAN = 2048
TAPS = 16
DSPAN = 3
LANES = 128
RADIX = NCHAN // LANES
GROUP = 8
TILE = 256
NTILE = NCHAN // TILE
CHUNK = 6
GRANT = 16 * 1024 * 1024

f32 = jnp.float32
bf16 = jnp.bfloat16


def split_pair(table):
    table = np.asarray(table, np.float32)
    high = table.astype(jnp.bfloat16)
    low = (table - high.astype(np.float32)).astype(jnp.bfloat16)
    return np.stack([high, low])


def make_tables():
    length = TAPS * NCHAN
    position = np.arange(length, dtype=np.float64)
    window = 0.54 - 0.46 * np.cos(2.0 * np.pi * position / (length - 1))
    shaped = np.sinc((position - (length - 1) / 2.0) / NCHAN) * window
    shaped = shaped * np.sqrt(NCHAN / np.sum(shaped * shaped))
    coeffs = shaped.reshape(TAPS * RADIX, LANES).astype(np.float32)
    rows = np.arange(RADIX)
    angle = 2.0 * np.pi * np.outer(rows, rows) / RADIX
    eye = np.eye(GROUP)
    cos_one, sin_one = np.kron(eye, np.cos(angle)), np.kron(eye, np.sin(angle))
    first = split_pair(np.block([[cos_one, sin_one], [-sin_one, cos_one]]))
    lanes = np.arange(LANES)
    angle = 2.0 * np.pi * np.outer(rows, lanes) / NCHAN
    twist = np.stack([np.tile(np.cos(angle), (GROUP, 1)), np.tile(np.sin(angle), (GROUP, 1))])
    angle = 2.0 * np.pi * np.outer(lanes, lanes) / LANES
    scale = 1.0 / math.sqrt(NCHAN)
    cos_two, sin_two = scale * np.cos(angle), scale * np.sin(angle)
    second = split_pair(np.block([[cos_two, -sin_two], [sin_two, cos_two]]))
    low_count = TILE // RADIX
    order = np.zeros((TILE, TILE), np.float32)
    for k_one in range(RADIX):
        for k_low in range(low_count):
            order[k_low * RADIX + k_one, k_one * low_count + k_low] = 1.0
    return coeffs, first, twist.astype(np.float32), second, order.astype(jnp.bfloat16)


def halves(value):
    high = value.astype(bf16)
    return high, (value - high.astype(f32)).astype(bf16)


def dot(left, right):
    return jnp.dot(left, right, preferred_element_type=f32)


def roll_left(value, steps):
    width = value.shape[-1]
    return pltpu.roll(value, (width - steps) % width, axis=value.ndim - 1)


def detect(ext_ref, coeffs_ref, first_ref, twist_ref, second_ref, weighted_ref, det_ref):
    for half in range(RADIX // 8):
        taps = [coeffs_ref[tap * RADIX + half * 8 : tap * RADIX + half * 8 + 8] for tap in range(TAPS)]

        def weigh(group, carry):
            for plane in range(4):
                pol, part = divmod(plane, 2)
                for inner in range(GROUP):
                    start = pl.multiple_of((group * GROUP + inner) * RADIX + half * 8, 8)
                    total = None
                    for tap in range(TAPS):
                        term = taps[tap] * ext_ref[plane, pl.ds(start + tap * RADIX, 8)]
                        total = term if total is None else total + term
                    row = part * GROUP * RADIX + inner * RADIX + half * 8
                    weighted_ref[group, row : row + 8, pol * LANES : (pol + 1) * LANES] = total
            return carry

        lax.fori_loop(0, det_ref.shape[0] // (GROUP * RADIX), weigh, 0)

    span = GROUP * RADIX
    twist_cos, twist_sin = twist_ref[0], twist_ref[1]
    for group in range(det_ref.shape[0] // (GROUP * RADIX)):
        high, low = halves(weighted_ref[group])
        mixed = dot(first_ref[0], high) + dot(first_ref[0], low) + dot(first_ref[1], high)
        energy = None
        for pol in range(2):
            real = mixed[:span, pol * LANES : (pol + 1) * LANES]
            imag = mixed[span:, pol * LANES : (pol + 1) * LANES]
            turned = jnp.concatenate(
                [real * twist_cos + imag * twist_sin, imag * twist_cos - real * twist_sin], axis=1
            )
            high, low = halves(turned)
            final = dot(high, second_ref[0]) + dot(low, second_ref[0]) + dot(high, second_ref[1])
            square = final * final
            power = square[:, :LANES] + square[:, LANES:]
            energy = power if energy is None else energy + power
        det_ref[group * span : (group + 1) * span] = energy.astype(bf16).astype(f32)


def early_kernel(delays_ref, mask_ref, order_ref, x_ref, coeffs_ref, first_ref, twist_ref, second_ref,
                 rel_ref, base_ref, reach_ref, late_ref, ext_ref, weighted_ref):
    start = x_ref.shape[1] - ext_ref.shape[1]
    for plane in range(4):
        ext_ref[plane] = x_ref[plane, start:].astype(f32)
    detect(ext_ref, coeffs_ref, first_ref, twist_ref, second_ref, weighted_ref, late_ref)
    order = order_ref[...]
    for tile in range(NTILE):
        here = delays_ref[:, tile * TILE : (tile + 1) * TILE]
        least = here[:, TILE - 1 : TILE]
        live = mask_ref[:, tile * TILE : (tile + 1) * TILE] > 0
        rel = jnp.where(live, here - least, -1).astype(f32).astype(bf16)
        rel_ref[:, tile * TILE : (tile + 1) * TILE] = dot(rel, order).astype(bf16)
        base_ref[tile] = jnp.broadcast_to(least, base_ref.shape[1:])
        reach_ref[tile] = jnp.max(here[:, 0:1] - least)


def main_kernel(reach_ref, x_ref, hist_ref, coeffs_ref, first_ref, twist_ref, second_ref, rel_ref,
                base_ref, late_ref, out_ref, ext_ref, weighted_ref, first_det_ref, det_ref, tile_ref, acc_ref):
    frames = x_ref.shape[1] // RADIX
    past = (TAPS - 1) * RADIX
    middle = frames // 2 * RADIX
    for plane in range(4):
        ext_ref[plane, :past] = hist_ref[plane].astype(f32)
        ext_ref[plane, past:] = x_ref[plane, :middle].astype(f32)
    tile_ref[...] = jnp.zeros_like(tile_ref)
    detect(ext_ref, coeffs_ref, first_ref, twist_ref, second_ref, weighted_ref, first_det_ref)
    det_ref[:middle] = first_det_ref[...]
    det_ref[middle:] = late_ref[...]

    width = LANES // 8
    lane_group = lax.broadcasted_iota(jnp.int32, (frames, LANES), 1) // width
    for half in range(RADIX // 8):
        rows = [det_ref[pl.ds(half * 8 + index, frames, stride=RADIX), :] for index in range(8)]
        for bit in (4, 2, 1):
            upper = (lane_group & bit) != 0
            for index in range(8):
                if index & bit:
                    continue
                one, two = rows[index], rows[index + bit]
                rows[index] = jnp.where(upper, pltpu.roll(two, bit * width, axis=1), one)
                rows[index + bit] = jnp.where(upper, two, roll_left(one, bit * width))
        for tile in range(NTILE):
            tile_ref[tile, DSPAN * frames :, half * LANES : (half + 1) * LANES] = rows[tile].astype(bf16)

    trials = rel_ref.shape[0]
    acc_ref[...] = jnp.zeros_like(acc_ref)
    most = reach_ref[0]
    for tile in range(1, NTILE):
        most = jnp.maximum(most, reach_ref[tile])
    steps = most // CHUNK + 1
    one = jnp.ones((trials, TILE), bf16)
    zero = jnp.zeros((trials, TILE), bf16)

    def add_chunk(step, carry):
        lowest = (steps - 1 - step) * CHUNK
        for tile in range(NTILE):
            rel = rel_ref[:, tile * TILE : (tile + 1) * TILE]
            chosen = jnp.concatenate(
                [
                    jnp.where(rel == (lowest + offset).astype(f32).astype(bf16), one, zero)
                    for offset in range(CHUNK)
                ],
                axis=0,
            )
            sums = lax.dot_general(
                chosen, tile_ref[tile], (((1,), (1,)), ((), ())), preferred_element_type=f32
            )
            acc = roll_left(acc_ref[tile], CHUNK) + sums[:trials]
            for offset in range(1, CHUNK):
                acc = acc + roll_left(sums[offset * trials : (offset + 1) * trials], offset)
            acc_ref[tile] = acc
        return carry

    lax.fori_loop(0, steps, add_chunk, 0)

    total = None
    for tile in range(NTILE):
        base = base_ref[tile]
        value = acc_ref[tile]
        bit = 1
        while bit <= DSPAN * frames:
            value = jnp.where((base & bit) != 0, roll_left(value, bit), value)
            bit *= 2
        total = value if total is None else total + value
    for device in range(out_ref.shape[0]):
        out_ref[device] = total


def stats_kernel(where_ref, parts_ref, mask_ref, zscore_ref, stats_ref):
    count, trials, width = parts_ref.shape
    frames = zscore_ref.shape[0]
    share = width // frames
    lane = lax.broadcasted_iota(jnp.int32, (trials, width), 1)
    block = lane // frames
    sums = [None] * (count // share)

    def put(index, value):
        sums[index] = value if sums[index] is None else sums[index] + value

    for device in range(count):
        part = parts_ref[device]
        turn = frames * ((device + 1) % share)
        if turn:
            part = pltpu.roll(part, turn, axis=1)
        group, within = divmod(device, share)
        stays = block <= within
        put(group, jnp.where(stays, part, 0.0))
        if group > 0 and within < share - 1:
            put(group - 1, jnp.where(stays, 0.0, part))
    total_frames = float(count * frames)
    whole, peak = sums[0], sums[0]
    for part in sums[1:]:
        whole = whole + part
        peak = jnp.maximum(peak, part)
    average = jnp.sum(whole, axis=1, keepdims=True) / total_frames
    peak_value = jnp.max(peak, axis=1, keepdims=True)
    squares = None
    mine = jnp.zeros((trials, width), f32)
    own_group = where_ref[0] // share
    for index, part in enumerate(sums):
        centred = part - average
        square = centred * centred
        squares = square if squares is None else squares + square
        mine = jnp.where(own_group == index, centred, mine)
    variance = jnp.sum(squares, axis=1, keepdims=True) / total_frames
    deviation = jnp.sqrt(variance + 1e-05)
    own_block = where_ref[0] % share
    scaled = (mine / deviation).T
    picked = None
    for index in range(share):
        piece = jnp.where(own_block == index, scaled[index * frames : (index + 1) * frames], 0.0)
        picked = piece if picked is None else picked + piece
    zscore_ref[...] = picked
    live = jnp.sum(mask_ref[...].astype(f32), axis=1, keepdims=True)
    live = jnp.maximum(live, 1.0)
    row = lax.broadcasted_iota(jnp.int32, (trials, width), 0)
    for index, column in enumerate((average / live, deviation / live, (peak_value - average) / deviation)):
        spread = jnp.where(row == lane, column, 0.0)
        stats_ref[index : index + 1, :] = jnp.sum(spread, axis=0, keepdims=True)[:, :trials]


def per_device(voltage, delays, chan_mask):
    frames = voltage.shape[2] // NCHAN
    trials = delays.shape[0]
    coeffs, first, twist, second, order = make_tables()
    framed = voltage.reshape(4, frames * RADIX, LANES)
    count = lax.axis_size("tm")
    hist = lax.ppermute(
        framed[:, (frames - TAPS + 1) * RADIX :], "tm", [(i, i + 1) for i in range(count - 1)]
    )
    mask_row = chan_mask.reshape(1, NCHAN)
    vmem = pl.BlockSpec(memory_space=pltpu.VMEM)
    smem = pl.BlockSpec(memory_space=pltpu.SMEM)
    half = frames // 2
    rel, base, reach, late = pl.pallas_call(
        early_kernel,
        name="early",
        compiler_params=pltpu.CompilerParams(vmem_limit_bytes=GRANT),
        out_shape=(
            jax.ShapeDtypeStruct((trials, NCHAN), bf16),
            jax.ShapeDtypeStruct((NTILE, trials, LANES), jnp.int32),
            jax.ShapeDtypeStruct((NTILE,), jnp.int32),
            jax.ShapeDtypeStruct((half * RADIX, LANES), f32),
        ),
        in_specs=[vmem] * 8,
        out_specs=(vmem, vmem, smem, vmem),
        scratch_shapes=[
            pltpu.VMEM((4, (half + TAPS - 1) * RADIX, LANES), f32),
            pltpu.VMEM((half // GROUP, 2 * GROUP * RADIX, 2 * LANES), f32),
        ],
    )(delays, mask_row, order, framed, coeffs, first, twist, second)
    window = (DSPAN + 1) * frames
    partial = pl.pallas_call(
        main_kernel,
        name="channelize",
        compiler_params=pltpu.CompilerParams(vmem_limit_bytes=GRANT),
        out_shape=jax.ShapeDtypeStruct((count, trials, window), f32),
        in_specs=[smem] + [vmem] * 9,
        out_specs=vmem,
        scratch_shapes=[
            pltpu.VMEM((4, (half + TAPS - 1) * RADIX, LANES), f32),
            pltpu.VMEM((half // GROUP, 2 * GROUP * RADIX, 2 * LANES), f32),
            pltpu.VMEM((half * RADIX, LANES), f32),
            pltpu.VMEM((frames * RADIX, LANES), f32),
            pltpu.VMEM((NTILE, window, TILE), bf16),
            pltpu.VMEM((NTILE, trials, window), f32),
        ],
    )(reach, framed, hist, coeffs, first, twist, second, rel, base, late)
    parts = lax.all_to_all(partial, "tm", 0, 0)
    here = lax.axis_index("tm").astype(jnp.int32).reshape(1)
    zscore, trial_stats = pl.pallas_call(
        stats_kernel,
        name="normalize",
        compiler_params=pltpu.CompilerParams(vmem_limit_bytes=GRANT),
        out_shape=(
            jax.ShapeDtypeStruct((frames, trials), f32),
            jax.ShapeDtypeStruct((3, trials), f32),
        ),
        in_specs=[smem, vmem, vmem],
        out_specs=(vmem, vmem),
    )(here, parts, mask_row)
    return zscore.T, trial_stats


def solution(mesh):
    in_specs = (P(None, None, ("beam", "tm")), P(), P("beam"))
    out_specs = (P(None, ("beam", "tm")), P(None, "beam"))
    return jax.shard_map(
        per_device, mesh=mesh, in_specs=in_specs, out_specs=out_specs, check_vma=False
    )
```
